256 devices in a mesh: frame: 32 (over y, z_hi, core), pos: 8 (over z_lo, x).
Axes of the slice: x: 4, y: 4, z: 8 (z_hi: 4, z_lo: 2; z = z_hi * 2 + z_lo), core: 2. Of those that a mesh axis runs over, the one named last changes fastest.
Arguments:
- spatial_qkv: bfloat16 [2, 32, 1536, 3, 1152], P(None, 'frame', 'pos'), may hold values from -9 to 9
- residual: bfloat16 [2, 32, 1536, 1152], P(None, 'frame', 'pos'), may hold values from -0.59765625 to 0.59765625
- spatial_gate: float32 [2, 1152], replicated, may hold values from 0.5 to 2
- spatial_proj: bfloat16 [1152, 1152], replicated, may hold values from -0.1875 to 0.1875
- spatial_qgain: float32 [72], replicated, may hold values from 0.5 to 8
- spatial_kgain: float32 [72], replicated, may hold values from 0.5 to 8
- temporal_shift: float32 [2, 1152], replicated, may hold values from -3 to 3
- temporal_scale: float32 [2, 1152], replicated, may hold values from -0.5 to 0.5
- temporal_qkv: bfloat16 [1152, 3456], replicated, as said below
- temporal_qgain: float32 [72], replicated, may hold values from 0.6 to 6
- temporal_kgain: float32 [72], replicated, may hold values from 0.6 to 6
Outputs:
- temporal_out: bfloat16 [2, 32, 1536, 1152], P(None, 'frame', 'pos')
The draws below stay inside these ranges and needn't reach their ends.
Inputs may be any that keep to these rules, and one draw needn't show every extreme that they name: `temporal_qkv`: entries are of the size of a weight with fan-in 1152.
All inputs are finite; a program needn't handle non-finite values.
Results may differ from the reference program's by a relative error of at most 0.028.
The reference program's roundings to bfloat16 on the way count: a program that leaves them out, or rounds other values in their place, can miss the bound.
Values may be sent and summed in bfloat16 or wider, within the bound.
A program may use at most 128 MiB of HBM per device.

```python
import math
import jax
import jax.numpy as jnp
from jax import lax

HEADS = 16
HEAD_DIM = 72
D = 1152
VIDEOS = 2
FRAMES = 32
POSITIONS = 1536


def gain_pair(key, stream):
    key_query, key_keys = jax.random.split(jax.random.fold_in(key, stream))
    query_gain = jax.random.uniform(key_query, (HEAD_DIM,), jnp.float32, 0.6, 1.6)
    keys_gain = jax.random.uniform(key_keys, (HEAD_DIM,), jnp.float32, 0.6, 1.6)
    return (query_gain, keys_gain)


def draw_spatial_qgain(key, part):
    return gain_pair(key, 101)[0]


def draw_spatial_kgain(key, part):
    return gain_pair(key, 101)[1]


def draw_temporal_qgain(key, part):
    return gain_pair(key, 202)[0]


def draw_temporal_kgain(key, part):
    return gain_pair(key, 202)[1]


def draw_spatial_qkv(key, part):
    key_base = jax.random.fold_in(jax.random.fold_in(key, 303), 0)
    full_shape = (VIDEOS, FRAMES, POSITIONS, 3, HEADS, HEAD_DIM)
    values = jnp.clip(jax.random.normal(key_base, full_shape, jnp.float32), -6.0, 6.0)
    return values.reshape(VIDEOS, FRAMES, POSITIONS, 3, D).astype(jnp.bfloat16)


def draw_temporal_qkv(key, part):
    key_base = jax.random.fold_in(jax.random.fold_in(key, 404), 0)
    weights = jnp.clip(jax.random.normal(key_base, (D, 3, HEADS, HEAD_DIM), jnp.float32), -4.0, 4.0) / math.sqrt(D)
    return weights.reshape(D, 3 * D).astype(jnp.bfloat16)


def levels(stream_key, extent, pieces, low, high):
    level = 1.0
    for dim, shards_of in pieces:
        heights = jax.random.uniform(jax.random.fold_in(jax.random.fold_in(stream_key, 6), dim), (shards_of,), jnp.float32, low / len(pieces), high / len(pieces))
        level = level * jnp.repeat(jnp.exp(heights), extent[dim] // shards_of).reshape((-1,) + (1,) * (len(extent) - 1 - dim))
    return level


def scatter_about(own_key, extent, width, most, pieces=(), held_as=jnp.bfloat16):
    drawn = jax.random.normal(own_key, extent, jnp.float32) * width
    if len(pieces) > 0:
        drawn = levels(own_key, extent, pieces, -0.22, 0.18) * drawn
    return jnp.clip(drawn, min=-most, max=most).astype(held_as)


def setup_inputs(seed: int = 0) -> dict:
    key_list = jax.random.split(jax.random.key(seed), 12)
    spatial_qkv = draw_spatial_qkv(jax.random.fold_in(key_list[11], 71), 0)
    residual = scatter_about(key_list[1], (VIDEOS, FRAMES, POSITIONS, D), 0.1, 0.59765625, ((1, 32), (2, 8)))
    spatial_gate = jnp.clip(jax.random.uniform(key_list[2], (VIDEOS, D), jnp.float32, 0.5, 2.0), 0.5, 2.0)
    spatial_proj = scatter_about(key_list[3], (D, D), D ** -0.5, 0.1875)
    spatial_qgain = draw_spatial_qgain(jax.random.fold_in(key_list[11], 71), 0)
    spatial_kgain = draw_spatial_kgain(jax.random.fold_in(key_list[11], 71), 0)
    temporal_shift = scatter_about(key_list[6], (VIDEOS, D), 0.5, 3.0, (), jnp.float32)
    temporal_scale = jnp.clip(jax.random.uniform(key_list[7], (VIDEOS, D), jnp.float32, -0.5, 0.5), -0.5, 0.5)
    temporal_qkv = draw_temporal_qkv(jax.random.fold_in(key_list[11], 71), 0)
    temporal_qgain = draw_temporal_qgain(jax.random.fold_in(key_list[11], 71), 0)
    temporal_kgain = draw_temporal_kgain(jax.random.fold_in(key_list[11], 71), 0)
    return {"spatial_qkv": spatial_qkv, "residual": residual, "spatial_gate": spatial_gate, "spatial_proj": spatial_proj, "spatial_qgain": spatial_qgain, "spatial_kgain": spatial_kgain, "temporal_shift": temporal_shift, "temporal_scale": temporal_scale, "temporal_qkv": temporal_qkv, "temporal_qgain": temporal_qgain, "temporal_kgain": temporal_kgain}


EPSILON = 1e-06

def head_norm(values, gain):
    widened = values.astype(jnp.float32)
    factor = lax.rsqrt(lax.optimization_barrier(jnp.mean(widened * widened, axis=-1, keepdims=True)) + EPSILON)
    return (widened * factor * gain).astype(jnp.bfloat16)

def softmax_weights(scores):
    row_top = lax.optimization_barrier(jnp.max(scores, axis=-1, keepdims=True))
    expons = jnp.exp(scores - row_top)
    return (expons / lax.optimization_barrier(jnp.sum(expons, axis=-1, keepdims=True))).astype(jnp.bfloat16)

def spatial_attend(element, query_gain, keys_gain):
    query_norm = head_norm(element[:, 0], query_gain)
    keys_norm = head_norm(element[:, 1], keys_gain)
    scores = jnp.einsum('qhd,khd->hqk', query_norm.astype(jnp.float32), keys_norm.astype(jnp.float32)) / math.sqrt(HEAD_DIM)
    weights = softmax_weights(scores)
    return jnp.einsum('hqk,khd->qhd', weights.astype(jnp.float32), element[:, 2].astype(jnp.float32)).astype(jnp.bfloat16)

def modulate(updated, shift_rows, scale_rows):
    widened = updated.astype(jnp.float32)
    centred = widened - lax.optimization_barrier(jnp.mean(widened, axis=-1, keepdims=True))
    spread = lax.optimization_barrier(jnp.mean(centred * centred, axis=-1, keepdims=True))
    scaled = centred * lax.rsqrt(spread + EPSILON) * (1.0 + scale_rows[:, None, None, :])
    return (scaled + shift_rows[:, None, None, :]).astype(jnp.bfloat16)

def temporal_attend(projected, query_gain, keys_gain):
    query_norm = head_norm(projected[:, :, :, 0], query_gain)
    keys_norm = head_norm(projected[:, :, :, 1], keys_gain)
    scores = jnp.einsum('bfphd,bgphd->bphfg', query_norm.astype(jnp.float32), keys_norm.astype(jnp.float32)) / math.sqrt(HEAD_DIM)
    weights = softmax_weights(scores)
    result = jnp.einsum('bphfg,bgphd->bfphd', weights.astype(jnp.float32), projected[:, :, :, 2].astype(jnp.float32))
    return result.astype(jnp.bfloat16).reshape(VIDEOS, FRAMES, POSITIONS, D)

def reference(spatial_qkv, residual, spatial_gate, spatial_proj, spatial_qgain, spatial_kgain, temporal_shift, temporal_scale, temporal_qkv, temporal_qgain, temporal_kgain):
    stacked = spatial_qkv.reshape(VIDEOS * FRAMES, POSITIONS, 3, HEADS, HEAD_DIM)
    attended = lax.map(lambda element: spatial_attend(element, spatial_qgain, spatial_kgain), stacked)
    mixed = jnp.dot(attended.reshape(VIDEOS * FRAMES * POSITIONS, D), spatial_proj, preferred_element_type=jnp.float32)
    mixed = mixed.reshape(VIDEOS, FRAMES, POSITIONS, D)
    updated = (residual.astype(jnp.float32) + spatial_gate[:, None, None, :] * mixed).astype(jnp.bfloat16)
    normed = modulate(updated, temporal_shift, temporal_scale)
    projected = jnp.dot(normed.reshape(VIDEOS * FRAMES * POSITIONS, D), temporal_qkv, preferred_element_type=jnp.float32)
    projected = projected.astype(jnp.bfloat16).reshape(VIDEOS, FRAMES, POSITIONS, 3, HEADS, HEAD_DIM)
    return temporal_attend(projected, temporal_qgain, temporal_kgain)
```

```python
import math

import jax
import jax.numpy as jnp
from jax import lax
from jax.experimental import pallas as pl
from jax.experimental.pallas import tpu as pltpu
from jax.sharding import PartitionSpec as P

EPSILON = 1e-06
MESH = pl.DeviceIdType.MESH
BF16 = jnp.bfloat16
F32 = jnp.float32
HEAD_DIM = 72
LANES = 128
SLAB = 4
LOG2E = 1.4426950408889634
SCORE_SCALE = LOG2E / math.sqrt(HEAD_DIM)


def norm_rows(values, gain):
    mean = jnp.sum(values * values, axis=0, keepdims=True) * (1.0 / HEAD_DIM)
    return values * lax.rsqrt(mean + EPSILON) * gain


def spatial_kernel(
    x_ref,
    residual_ref,
    gate_ref,
    proj_ref,
    qgain_ref,
    kgain_ref,
    shift_ref,
    scale_ref,
    out_ref,
    wide,
    send,
    recv,
    queries,
    keys,
    values,
    scores,
    outgoing,
    attended,
    send_sem,
    recv_sem,
    back_send_sem,
    back_recv_sem,
):
    me = lax.axis_index("pos")
    odd = lax.rem(me, 2)
    barrier = pltpu.get_barrier_semaphore()
    for r in range(1, 8):
        pl.semaphore_signal(
            barrier, inc=1, device_id={"pos": lax.rem(me + r, 8)}, device_id_type=MESH
        )

    swap = jnp.zeros((64, LANES), jnp.int32) + odd == 1

    def turn(j, carry):
        columns = pl.ds(pl.multiple_of(j * LANES, LANES), LANES)
        for t in range(3):
            first = x_ref[0, t, :, columns].astype(F32)
            second = x_ref[1, t, :, columns].astype(F32)
            low, high = first[128:], second[:64]
            block = jnp.concatenate(
                [first[:128], jnp.where(swap, high, low), jnp.where(swap, low, high), second[64:]],
                axis=0,
            )
            wide[t, columns, :] = block.T
        return carry

    lax.fori_loop(0, 9, turn, 0)

    def exchange(h, r):
        peer = lax.rem(me + r, 8)
        return pltpu.make_async_remote_copy(
            src_ref=send.at[2 * peer + h],
            dst_ref=recv.at[h, r],
            send_sem=send_sem.at[h, r],
            recv_sem=recv_sem.at[h, r],
            device_id={"pos": peer},
            device_id_type=MESH,
        )

    for h in range(2):

        def pack(d, carry):
            rows = pl.ds(pl.multiple_of(d * 144 + 72 * h, 8), HEAD_DIM)
            send[2 * d + h, 0] = norm_rows(wide[0, rows, :], qgain_ref[...]).astype(BF16)
            send[2 * d + h, 1] = norm_rows(wide[1, rows, :], kgain_ref[...]).astype(BF16)
            send[2 * d + h, 2] = wide[2, rows, :].astype(BF16)
            return carry

        lax.fori_loop(0, 8, pack, 0)
        if h == 0:
            pl.semaphore_wait(barrier, 7)
        for r in range(1, 8):
            exchange(h, r).start()
    for h in range(2):
        recv[h, 0] = send[2 * me + h]
    for v in range(2):
        values[v, 72:80, :] = jnp.ones((8, 1536), BF16)

    lane = lax.broadcasted_iota(jnp.int32, (HEAD_DIM, LANES), 1)
    straight = (lane < 64) == ((jnp.zeros((HEAD_DIM, LANES), jnp.int32) + odd) == 0)

    def give_back(h, r):
        return pltpu.make_async_remote_copy(
            src_ref=outgoing.at[h, r],
            dst_ref=attended.at[2 * me + h],
            send_sem=back_send_sem.at[h, r],
            recv_sem=back_recv_sem.at[h, r],
            device_id={"pos": lax.rem(me + 8 - r, 8)},
            device_id_type=MESH,
        )

    for h in range(2):
        for i in range(4):
            for r in (2 * i, 2 * i + 1):
                if r > 0:
                    exchange(h, r).wait_recv()
            span = slice(384 * i, 384 * i + 384)
            for t in range(3):
                a, b = recv[h, 2 * i, t], recv[h, 2 * i + 1, t]
                amid, bmid = a[:, 128:256].astype(F32), b[:, 128:256].astype(F32)
                mids = (
                    jnp.where(straight, amid, bmid).astype(BF16),
                    jnp.where(straight, bmid, amid).astype(BF16),
                )
                for v in range(2):
                    edge = slice(256 * v, 256 * v + 128)
                    pieces = (a[:, edge], b[:, edge], mids[v])
                    for n, piece in enumerate(pieces):
                        place = slice(384 * i + 128 * n, 384 * i + 128 * n + 128)
                        if t == 0:
                            queries[v, :, place] = piece
                        elif t == 1:
                            keys[v, place, :] = piece.T
                        else:
                            values[v, 0:72, place] = piece
        for g in range(2):
            results = []
            for v in range(2):
                block = queries[v, :, 768 * g : 768 * g + 768]
                top = None
                for c in range(6):
                    part = jnp.dot(
                        keys[v, 256 * c : 256 * c + 256, :], block, preferred_element_type=F32
                    )
                    scores[v, 256 * c : 256 * c + 256, :] = part
                    part_top = jnp.max(part.reshape(32, 8, 768), axis=0)
                    top = part_top if top is None else jnp.maximum(top, part_top)
                top = jnp.max(top, axis=0, keepdims=True) * SCORE_SCALE
                total = None
                for c in range(6):
                    expons = jnp.exp2(
                        scores[v, 256 * c : 256 * c + 256, :] * SCORE_SCALE - top
                    ).astype(BF16)
                    part = jnp.dot(
                        values[v, :, 256 * c : 256 * c + 256], expons, preferred_element_type=F32
                    )
                    total = part if total is None else total + part
                results.append(total[:72] / total[72:73])
            for i in (2 * g, 2 * g + 1):
                base = 384 * (i - 2 * g)
                mid0 = results[0][:, base + 256 : base + 384]
                mid1 = results[1][:, base + 256 : base + 384]
                for n in range(2):
                    r = 2 * i + n
                    edge = slice(base + 128 * n, base + 128 * n + 128)
                    if n == 0:
                        mid = jnp.where(straight, mid0, mid1)
                    else:
                        mid = jnp.where(straight, mid1, mid0)
                    pieces = (results[0][:, edge], mid, results[1][:, edge])
                    for m, piece in enumerate(pieces):
                        place = slice(128 * m, 128 * m + 128)
                        if r == 0:
                            attended[2 * me + h, :, place] = piece.astype(BF16)
                        else:
                            outgoing[h, r, :, place] = piece.astype(BF16)
                    if r > 0:
                        give_back(h, r).start()

    def arrived(h, r):
        return pltpu.make_async_remote_copy(
            src_ref=outgoing.at[h, r],
            dst_ref=attended.at[2 * lax.rem(me + r, 8) + h],
            send_sem=back_send_sem.at[h, r],
            recv_sem=back_recv_sem.at[h, r],
            device_id={"pos": lax.rem(me + r, 8)},
            device_id_type=MESH,
        )

    for h in range(2):
        for r in range(1, 8):
            arrived(h, r).wait_recv()
    for n in range(16):
        wide[0, 72 * n : 72 * n + 72, :] = attended[n].astype(F32)
    gate_odd = jnp.zeros((LANES, 1152), jnp.int32) + odd == 1
    for tile in range(3):
        rows = wide[0, :, 128 * tile : 128 * tile + 128].T
        if tile == 1:
            rows = jnp.where(gate_odd, jnp.concatenate([rows[64:], rows[:64]], axis=0), rows)
        mixed = jnp.dot(rows.astype(BF16), proj_ref[...], preferred_element_type=F32)
        for half in range(2):
            start = 128 * tile + 64 * half
            v, p = divmod(start, 192)
            updated = (
                residual_ref[v, p : p + 64, :].astype(F32)
                + gate_ref[v : v + 1, :] * mixed[64 * half : 64 * half + 64]
            ).astype(BF16)
            widened = updated.astype(F32)
            centred = widened - jnp.mean(widened, axis=-1, keepdims=True)
            spread = jnp.mean(centred * centred, axis=-1, keepdims=True)
            scaled = centred * lax.rsqrt(spread + EPSILON) * (1.0 + scale_ref[v : v + 1, :])
            normed = (scaled + shift_ref[v : v + 1, :]).astype(BF16)
            out_ref[start // SLAB : start // SLAB + 16] = normed.reshape(16, SLAB, 1152)
    for h in range(2):
        for r in range(1, 8):
            exchange(h, r).wait_send()
            give_back(h, r).wait_send()


def temporal_kernel(
    rows_ref,
    weight_ref,
    qgain_ref,
    kgain_ref,
    out_ref,
    weight,
    recv,
    turned,
    result,
    outgoing,
    back,
    weight_sem,
    send_sem,
    recv_sem,
    back_send_sem,
    back_recv_sem,
):
    me = lax.axis_index("frame")
    load = pltpu.make_async_copy(weight_ref, weight, weight_sem)
    load.start()
    barrier = pltpu.get_barrier_semaphore()

    def greet(r, carry):
        pl.semaphore_signal(
            barrier, inc=1, device_id={"frame": lax.rem(me + r, 32)}, device_id_type=MESH
        )
        return carry

    lax.fori_loop(1, 32, greet, 0)
    pl.semaphore_wait(barrier, 31)

    for i in range(3):

        def give(r, carry):
            peer = lax.rem(me + r, 32)
            pltpu.make_async_remote_copy(
                src_ref=rows_ref.at[3 * peer + i],
                dst_ref=recv.at[i, r],
                send_sem=send_sem.at[i],
                recv_sem=recv_sem.at[i],
                device_id={"frame": peer},
                device_id_type=MESH,
            ).start()
            return carry

        lax.fori_loop(1, 32, give, 0)
        recv[i, 0] = rows_ref[3 * me + i]

    def all_of(buffer, i, send_sems, recv_sems):
        return pltpu.make_async_remote_copy(
            src_ref=buffer.at[i, pl.ds(1, 31)],
            dst_ref=buffer.at[i, pl.ds(1, 31)],
            send_sem=send_sems.at[i],
            recv_sem=recv_sems.at[i],
            device_id={"frame": lax.rem(me + 1, 32)},
            device_id_type=MESH,
        )

    load.wait()
    row = lax.broadcasted_iota(jnp.int32, (LANES, LANES), 0)
    column = lax.broadcasted_iota(jnp.int32, (LANES, LANES), 1)
    same = lax.rem(row, SLAB) == lax.rem(column, SLAB)
    for i in range(3):
        all_of(recv, i, send_sem, recv_sem).wait_recv()
        tokens = recv[i].reshape(LANES, 1152)
        for t in range(3):
            projected = jnp.dot(
                tokens, weight[:, 1152 * t : 1152 * t + 1152], preferred_element_type=F32
            ).astype(BF16)
            turned[t] = projected.astype(F32).T
        for n in range(16):
            head = slice(72 * n, 72 * n + 72)
            query = norm_rows(turned[0, head, :], qgain_ref[...]).astype(BF16)
            key = norm_rows(turned[1, head, :], kgain_ref[...]).astype(BF16)
            score = lax.dot_general(
                key, query, (((0,), (0,)), ((), ())), preferred_element_type=F32
            )
            score = jnp.where(same, score * SCORE_SCALE, -1e30)
            expons = jnp.exp2(score - jnp.max(score, axis=0, keepdims=True))
            share = (expons / jnp.sum(expons, axis=0, keepdims=True)).astype(BF16)
            result[head, :] = jnp.dot(
                turned[2, head, :].astype(BF16), share, preferred_element_type=F32
            )
        outgoing[i] = result[...].T.astype(BF16).reshape(32, SLAB, 1152)

        def give_back(r, carry):
            pltpu.make_async_remote_copy(
                src_ref=outgoing.at[i, r],
                dst_ref=back.at[i, r],
                send_sem=back_send_sem.at[i],
                recv_sem=back_recv_sem.at[i],
                device_id={"frame": lax.rem(me + 32 - r, 32)},
                device_id_type=MESH,
            ).start()
            return carry

        lax.fori_loop(1, 32, give_back, 0)
        out_ref[3 * me + i] = outgoing[i, 0]
    for i in range(3):
        all_of(back, i, back_send_sem, back_recv_sem).wait_recv()

        def place(r, carry):
            out_ref[3 * lax.rem(me + r, 32) + i] = back[i, r]
            return carry

        lax.fori_loop(1, 32, place, 0)
    for i in range(3):
        all_of(recv, i, send_sem, recv_sem).wait_send()
        all_of(back, i, back_send_sem, back_recv_sem).wait_send()


def per_device(
    spatial_qkv,
    residual,
    spatial_gate,
    spatial_proj,
    spatial_qgain,
    spatial_kgain,
    temporal_shift,
    temporal_scale,
    temporal_qkv,
    temporal_qgain,
    temporal_kgain,
):
    vmem = pl.BlockSpec(memory_space=pltpu.VMEM)
    dma = pltpu.SemaphoreType.DMA
    split = jnp.transpose(spatial_qkv, (0, 1, 3, 2, 4)).reshape(2, 3, 192, 1152)
    modulated = pl.pallas_call(
        spatial_kernel,
        out_shape=jax.ShapeDtypeStruct((96, SLAB, 1152), BF16),
        in_specs=[vmem] * 8,
        out_specs=vmem,
        scratch_shapes=[
            pltpu.VMEM((3, 1152, 384), F32),
            pltpu.VMEM((16, 3, 72, 384), BF16),
            pltpu.VMEM((2, 8, 3, 72, 384), BF16),
            pltpu.VMEM((2, 72, 1536), BF16),
            pltpu.VMEM((2, 1536, 72), BF16),
            pltpu.VMEM((2, 80, 1536), BF16),
            pltpu.VMEM((2, 1536, 768), F32),
            pltpu.VMEM((2, 8, 72, 384), BF16),
            pltpu.VMEM((16, 72, 384), BF16),
            dma((2, 8)),
            dma((2, 8)),
            dma((2, 8)),
            dma((2, 8)),
        ],
        compiler_params=pltpu.CompilerParams(
            collective_id=0, has_side_effects=True, vmem_limit_bytes=56 * 1024 * 1024
        ),
        name="spatial",
    )(
        split,
        residual.reshape(2, 192, 1152),
        spatial_gate,
        spatial_proj,
        spatial_qgain.reshape(72, 1),
        spatial_kgain.reshape(72, 1),
        temporal_shift,
        temporal_scale,
    )
    result = pl.pallas_call(
        temporal_kernel,
        out_shape=jax.ShapeDtypeStruct((96, SLAB, 1152), BF16),
        in_specs=[vmem, pl.BlockSpec(memory_space=pl.ANY), vmem, vmem],
        out_specs=vmem,
        scratch_shapes=[
            pltpu.VMEM((1152, 3456), BF16),
            pltpu.VMEM((3, 32, SLAB, 1152), BF16),
            pltpu.VMEM((3, 1152, LANES), F32),
            pltpu.VMEM((1152, LANES), F32),
            pltpu.VMEM((3, 32, SLAB, 1152), BF16),
            pltpu.VMEM((3, 32, SLAB, 1152), BF16),
            dma,
            dma((3,)),
            dma((3,)),
            dma((3,)),
            dma((3,)),
        ],
        compiler_params=pltpu.CompilerParams(
            collective_id=1, has_side_effects=True, vmem_limit_bytes=56 * 1024 * 1024
        ),
        name="temporal",
    )(modulated, temporal_qkv, temporal_qgain.reshape(72, 1), temporal_kgain.reshape(72, 1))
    return result.reshape(2, 1, 192, 1152)


def solution(mesh):
    return jax.shard_map(
        per_device,
        mesh=mesh,
        in_specs=(
            P(None, "frame", "pos", None, None),
            P(None, "frame", "pos", None),
            P(),
            P(),
            P(),
            P(),
            P(),
            P(),
            P(),
            P(),
            P(),
        ),
        out_specs=P(None, "frame", "pos", None),
        check_vma=False,
    )
```

```python
import math

import jax
import jax.numpy as jnp
from jax import lax
from jax.experimental import pallas as pl
from jax.experimental.pallas import tpu as pltpu
from jax.sharding import PartitionSpec as P

EPSILON = 1e-06
MESH = pl.DeviceIdType.MESH
BF16 = jnp.bfloat16
F32 = jnp.float32
HEAD_DIM = 72
LANES = 128
SLAB = 4
LOG2E = 1.4426950408889634
SCORE_SCALE = LOG2E / math.sqrt(HEAD_DIM)


def norm_rows(values, gain):
    mean = jnp.sum(values * values, axis=0, keepdims=True) * (1.0 / HEAD_DIM)
    return values * lax.rsqrt(mean + EPSILON) * gain


def fused_kernel(
    x_ref,
    residual_ref,
    proj_ref,
    weight_ref,
    gate_ref,
    shift_ref,
    scale_ref,
    spatial_qgain_ref,
    spatial_kgain_ref,
    temporal_qgain_ref,
    temporal_kgain_ref,
    out_ref,
    taken,
    residual,
    proj,
    weight,
    gains,
    wide,
    send,
    recv,
    queries,
    keys,
    values,
    scores,
    outgoing,
    attended,
    slabs,
    slab_recv,
    turned,
    result,
    slab_outgoing,
    slab_back,
    load_sem,
    take_sem,
    send_sem,
    recv_sem,
    back_send_sem,
    back_recv_sem,
    slab_send_sem,
    slab_recv_sem,
    slab_back_send_sem,
    slab_back_recv_sem,
):
    me = lax.axis_index("pos")
    frame = lax.axis_index("frame")
    odd = lax.rem(me, 2)

    def take(s):
        j = lax.rem(me + 1 + s, 9)
        columns = pl.ds(pl.multiple_of(j * LANES, LANES), LANES)
        return pltpu.make_async_copy(
            x_ref.at[:, :, :, columns], taken.at[s], take_sem.at[s]
        )

    for s in range(9):
        take(s).start()
    barrier = pltpu.get_barrier_semaphore()
    for r in range(1, 8):
        pl.semaphore_signal(
            barrier, inc=1, device_id={"pos": lax.rem(me + r, 8)}, device_id_type=MESH
        )

    def greet(r, carry):
        pl.semaphore_signal(
            barrier, inc=1, device_id={"frame": lax.rem(frame + r, 32)}, device_id_type=MESH
        )
        return carry

    lax.fori_loop(1, 32, greet, 0)
    loads = [
        pltpu.make_async_copy(source, target, load_sem.at[n])
        for n, (source, target) in enumerate(
            ((residual_ref, residual), (proj_ref, proj), (weight_ref, weight))
        )
    ]
    for load in loads:
        load.start()
    for n, gain_ref in enumerate(
        (spatial_qgain_ref, spatial_kgain_ref, temporal_qgain_ref, temporal_kgain_ref)
    ):
        column = jnp.broadcast_to(gain_ref[...], (LANES, HEAD_DIM)).T
        for m in range(3):
            gains[n, :, 128 * m : 128 * m + 128] = column

    swap = jnp.zeros((64, LANES), jnp.int32) + odd == 1

    def turn(s):
        j = lax.rem(me + 1 + s, 9)
        rows = pl.ds(pl.multiple_of(j * LANES, LANES), LANES)
        for t in range(3):
            first = taken[s, 0, t].astype(F32)
            second = taken[s, 1, t].astype(F32)
            low, high = first[128:], second[:64]
            block = jnp.concatenate(
                [first[:128], jnp.where(swap, high, low), jnp.where(swap, low, high), second[64:]],
                axis=0,
            )
            wide[t, rows, :] = block.T

    def pack(d, h):
        rows = pl.ds(pl.multiple_of(d * 144 + 72 * h, 8), HEAD_DIM)
        send[2 * d + h, 0] = norm_rows(wide[0, rows, :], gains[0]).astype(BF16)
        send[2 * d + h, 1] = norm_rows(wide[1, rows, :], gains[1]).astype(BF16)
        send[2 * d + h, 2] = wide[2, rows, :].astype(BF16)

    def exchange(stage, peer, r):
        h = 0 if stage == 0 else 1
        part = ((0, 3), (1, 2), (0, 1))[stage]
        return pltpu.make_async_remote_copy(
            src_ref=send.at[2 * peer + h, pl.ds(*part)],
            dst_ref=recv.at[h, r, pl.ds(*part)],
            send_sem=send_sem.at[stage, r],
            recv_sem=recv_sem.at[stage, r],
            device_id={"pos": peer},
            device_id_type=MESH,
        )

    take(0).wait()
    turn(0)
    take(1).wait()
    turn(1)
    pl.semaphore_wait(barrier, 38)

    def feed(s, carry):
        @pl.when(s > 1)
        def _():
            take(s).wait()
            turn(s)

        j = lax.rem(me + 1 + s, 9)

        @pl.when(j >= 1)
        def _():
            peer = j - 1
            pack(peer, 0)
            exchange(0, peer, lax.rem(peer + 8 - me, 8)).start()

        return carry

    lax.fori_loop(1, 9, feed, 0)

    def feed_second(r, carry):
        peer = lax.rem(me + r, 8)
        pack(peer, 1)
        exchange(1, peer, r).start()
        return carry

    lax.fori_loop(1, 8, feed_second, 0)
    for r in range(1, 8):
        exchange(2, lax.rem(me + r, 8), r).start()
    for h in range(2):
        pack(me, h)
        recv[h, 0] = send[2 * me + h]
    for v in range(2):
        values[v, 72:80, :] = jnp.ones((8, 1536), BF16)

    lane = lax.broadcasted_iota(jnp.int32, (HEAD_DIM, LANES), 1)
    straight = (lane < 64) == ((jnp.zeros((HEAD_DIM, LANES), jnp.int32) + odd) == 0)

    def give_back(h, r):
        return pltpu.make_async_remote_copy(
            src_ref=outgoing.at[h, r],
            dst_ref=attended.at[2 * me + h],
            send_sem=back_send_sem.at[h, r],
            recv_sem=back_recv_sem.at[h, r],
            device_id={"pos": lax.rem(me + 8 - r, 8)},
            device_id_type=MESH,
        )

    def await_pair(stage, i):
        for r in (2 * i, 2 * i + 1):
            if r > 0:
                exchange(stage, lax.rem(me + r, 8), r).wait_recv()

    def spread(h, i, t):
        a, b = recv[h, 2 * i, t], recv[h, 2 * i + 1, t]
        amid, bmid = a[:, 128:256].astype(F32), b[:, 128:256].astype(F32)
        mids = (
            jnp.where(straight, amid, bmid).astype(BF16),
            jnp.where(straight, bmid, amid).astype(BF16),
        )
        for v in range(2):
            edge = slice(256 * v, 256 * v + 128)
            for n, piece in enumerate((a[:, edge], b[:, edge], mids[v])):
                place = slice(384 * i + 128 * n, 384 * i + 128 * n + 128)
                if t == 0:
                    queries[v, :, place] = piece
                elif t == 1:
                    keys[v, place, :] = piece.T
                else:
                    values[v, 0:72, place] = piece

    for h in range(2):
        for i in range(4):
            await_pair(h, i)
            spread(h, i, 1)
            spread(h, i, 2)
        for g in range(2):
            for i in (2 * g, 2 * g + 1):
                if h == 1:
                    await_pair(2, i)
                spread(h, i, 0)
            results = []
            for v in range(2):
                block = queries[v, :, 768 * g : 768 * g + 768]
                top = None
                for c in range(6):
                    part = jnp.dot(
                        keys[v, 256 * c : 256 * c + 256, :], block, preferred_element_type=F32
                    )
                    scores[v, 256 * c : 256 * c + 256, :] = part
                    part_top = jnp.max(part.reshape(32, 8, 768), axis=0)
                    top = part_top if top is None else jnp.maximum(top, part_top)
                top = jnp.max(top, axis=0, keepdims=True) * SCORE_SCALE
                total = None
                for c in range(6):
                    expons = jnp.exp2(
                        scores[v, 256 * c : 256 * c + 256, :] * SCORE_SCALE - top
                    ).astype(BF16)
                    part = jnp.dot(
                        values[v, :, 256 * c : 256 * c + 256], expons, preferred_element_type=F32
                    )
                    total = part if total is None else total + part
                results.append(total[:72] / total[72:73])
            for i in (2 * g, 2 * g + 1):
                base = 384 * (i - 2 * g)
                mid0 = results[0][:, base + 256 : base + 384]
                mid1 = results[1][:, base + 256 : base + 384]
                for n in range(2):
                    r = 2 * i + n
                    edge = slice(base + 128 * n, base + 128 * n + 128)
                    if n == 0:
                        mid = jnp.where(straight, mid0, mid1)
                    else:
                        mid = jnp.where(straight, mid1, mid0)
                    pieces = (results[0][:, edge], mid, results[1][:, edge])
                    for m, piece in enumerate(pieces):
                        place = slice(128 * m, 128 * m + 128)
                        if r == 0:
                            attended[2 * me + h, :, place] = piece.astype(BF16)
                        else:
                            outgoing[h, r, :, place] = piece.astype(BF16)
                    if r > 0:
                        give_back(h, r).start()

    def arrived(h, r):
        return pltpu.make_async_remote_copy(
            src_ref=outgoing.at[h, r],
            dst_ref=attended.at[2 * lax.rem(me + r, 8) + h],
            send_sem=back_send_sem.at[h, r],
            recv_sem=back_recv_sem.at[h, r],
            device_id={"pos": lax.rem(me + r, 8)},
            device_id_type=MESH,
        )

    for load in loads:
        load.wait()
    for h in range(2):
        for r in range(1, 8):
            arrived(h, r).wait_recv()
    for n in range(16):
        wide[0, 72 * n : 72 * n + 72, :] = attended[n].astype(F32)
    swap_rows = jnp.zeros((LANES, 1152), jnp.int32) + odd == 1

    def give_slab(i, r):
        peer = lax.rem(frame + r, 32)
        return pltpu.make_async_remote_copy(
            src_ref=slabs.at[32 * i + peer],
            dst_ref=slab_recv.at[i, r],
            send_sem=slab_send_sem.at[i],
            recv_sem=slab_recv_sem.at[i],
            device_id={"frame": peer},
            device_id_type=MESH,
        )

    for tile in range(3):
        rows = wide[0, :, 128 * tile : 128 * tile + 128].T
        if tile == 1:
            rows = jnp.where(swap_rows, jnp.concatenate([rows[64:], rows[:64]], axis=0), rows)
        mixed = jnp.dot(rows.astype(BF16), proj[...], preferred_element_type=F32)
        for half in range(2):
            start = 128 * tile + 64 * half
            v, p = divmod(start, 192)
            updated = (
                residual[v, p : p + 64, :].astype(F32)
                + gate_ref[v : v + 1, :] * mixed[64 * half : 64 * half + 64]
            ).astype(BF16)
            widened = updated.astype(F32)
            centred = widened - jnp.mean(widened, axis=-1, keepdims=True)
            spread_of = jnp.mean(centred * centred, axis=-1, keepdims=True)
            scaled = centred * lax.rsqrt(spread_of + EPSILON) * (1.0 + scale_ref[v : v + 1, :])
            normed = (scaled + shift_ref[v : v + 1, :]).astype(BF16)
            slabs[start // SLAB : start // SLAB + 16] = normed.reshape(16, SLAB, 1152)

        def give(r, carry):
            give_slab(tile, r).start()
            return carry

        lax.fori_loop(1, 32, give, 0)
        slab_recv[tile, 0] = slabs[32 * tile + frame]

    def all_of(buffer, send_sem, recv_sem):
        return pltpu.make_async_remote_copy(
            src_ref=buffer,
            dst_ref=buffer,
            send_sem=send_sem,
            recv_sem=recv_sem,
            device_id={"frame": lax.rem(frame + 1, 32)},
            device_id_type=MESH,
        )

    row = lax.broadcasted_iota(jnp.int32, (LANES, LANES), 0)
    column = lax.broadcasted_iota(jnp.int32, (LANES, LANES), 1)
    same = lax.rem(row, SLAB) == lax.rem(column, SLAB)
    for i in range(3):
        all_of(
            slab_recv.at[i, pl.ds(1, 31)], slab_send_sem.at[i], slab_recv_sem.at[i]
        ).wait_recv()
        tokens = slab_recv[i].reshape(LANES, 1152)
        for t in range(3):
            projected = jnp.dot(
                tokens, weight[:, 1152 * t : 1152 * t + 1152], preferred_element_type=F32
            ).astype(BF16)
            turned[t] = projected.astype(F32).T
        for n in range(16):
            head = slice(72 * n, 72 * n + 72)
            query = norm_rows(turned[0, head, :], gains[2, :, 0:128]).astype(BF16)
            key = norm_rows(turned[1, head, :], gains[3, :, 0:128]).astype(BF16)
            score = lax.dot_general(
                key, query, (((0,), (0,)), ((), ())), preferred_element_type=F32
            )
            score = jnp.where(same, score * SCORE_SCALE, -1e30)
            expons = jnp.exp2(score - jnp.max(score, axis=0, keepdims=True))
            share = (expons / jnp.sum(expons, axis=0, keepdims=True)).astype(BF16)
            result[head, :] = jnp.dot(
                turned[2, head, :].astype(BF16), share, preferred_element_type=F32
            )
        slab_outgoing[i] = result[...].T.astype(BF16).reshape(32, SLAB, 1152)

        def return_slab(r, carry):
            pltpu.make_async_remote_copy(
                src_ref=slab_outgoing.at[i, r],
                dst_ref=slab_back.at[32 * i + frame],
                send_sem=slab_back_send_sem.at[i],
                recv_sem=slab_back_recv_sem.at[i],
                device_id={"frame": lax.rem(frame + 32 - r, 32)},
                device_id_type=MESH,
            ).start()
            return carry

        lax.fori_loop(1, 32, return_slab, 0)
        slab_back[32 * i + frame] = slab_outgoing[i, 0]
    for stage in range(3):
        for r in range(1, 8):
            exchange(stage, lax.rem(me + r, 8), r).wait_send()
    for h in range(2):
        for r in range(1, 8):
            give_back(h, r).wait_send()
    for i in range(3):
        all_of(
            slab_back.at[pl.ds(32 * i, 31)], slab_back_send_sem.at[i], slab_back_recv_sem.at[i]
        ).wait_recv()
        out_ref[128 * i : 128 * i + 128, :] = slab_back[32 * i : 32 * i + 32].reshape(128, 1152)
    for i in range(3):
        all_of(
            slab_recv.at[i, pl.ds(1, 31)], slab_send_sem.at[i], slab_recv_sem.at[i]
        ).wait_send()
        all_of(
            slab_back.at[pl.ds(32 * i, 31)], slab_back_send_sem.at[i], slab_back_recv_sem.at[i]
        ).wait_send()


def per_device(
    spatial_qkv,
    residual,
    spatial_gate,
    spatial_proj,
    spatial_qgain,
    spatial_kgain,
    temporal_shift,
    temporal_scale,
    temporal_qkv,
    temporal_qgain,
    temporal_kgain,
):
    vmem = pl.BlockSpec(memory_space=pltpu.VMEM)
    anywhere = pl.BlockSpec(memory_space=pl.ANY)
    dma = pltpu.SemaphoreType.DMA
    split = jnp.transpose(spatial_qkv, (0, 1, 3, 2, 4)).reshape(2, 3, 192, 1152)
    result = pl.pallas_call(
        fused_kernel,
        out_shape=jax.ShapeDtypeStruct((384, 1152), BF16),
        in_specs=[anywhere] * 4 + [vmem] * 7,
        out_specs=vmem,
        scratch_shapes=[
            pltpu.VMEM((9, 2, 3, 192, LANES), BF16),
            pltpu.VMEM((2, 192, 1152), BF16),
            pltpu.VMEM((1152, 1152), BF16),
            pltpu.VMEM((1152, 3456), BF16),
            pltpu.VMEM((4, 72, 384), F32),
            pltpu.VMEM((3, 1152, 384), F32),
            pltpu.VMEM((16, 3, 72, 384), BF16),
            pltpu.VMEM((2, 8, 3, 72, 384), BF16),
            pltpu.VMEM((2, 72, 1536), BF16),
            pltpu.VMEM((2, 1536, 72), BF16),
            pltpu.VMEM((2, 80, 1536), BF16),
            pltpu.VMEM((2, 1536, 768), F32),
            pltpu.VMEM((2, 8, 72, 384), BF16),
            pltpu.VMEM((16, 72, 384), BF16),
            pltpu.VMEM((96, SLAB, 1152), BF16),
            pltpu.VMEM((3, 32, SLAB, 1152), BF16),
            pltpu.VMEM((3, 1152, LANES), F32),
            pltpu.VMEM((1152, LANES), F32),
            pltpu.VMEM((3, 32, SLAB, 1152), BF16),
            pltpu.VMEM((96, SLAB, 1152), BF16),
            dma((3,)),
            dma((9,)),
            dma((3, 8)),
            dma((3, 8)),
            dma((2, 8)),
            dma((2, 8)),
            dma((3,)),
            dma((3,)),
            dma((3,)),
            dma((3,)),
        ],
        compiler_params=pltpu.CompilerParams(
            collective_id=0, has_side_effects=True, vmem_limit_bytes=62 * 1024 * 1024
        ),
        name="fused",
    )(
        split,
        residual.reshape(2, 192, 1152),
        spatial_proj,
        temporal_qkv,
        spatial_gate,
        temporal_shift,
        temporal_scale,
        spatial_qgain.reshape(1, 72),
        spatial_kgain.reshape(1, 72),
        temporal_qgain.reshape(1, 72),
        temporal_kgain.reshape(1, 72),
    )
    return result.reshape(2, 1, 192, 1152)


def solution(mesh):
    return jax.shard_map(
        per_device,
        mesh=mesh,
        in_specs=(
            P(None, "frame", "pos", None, None),
            P(None, "frame", "pos", None),
            P(),
            P(),
            P(),
            P(),
            P(),
            P(),
            P(),
            P(),
            P(),
        ),
        out_specs=P(None, "frame", "pos", None),
        check_vma=False,
    )
```

```python
import math

import jax
import jax.numpy as jnp
from jax import lax
from jax.experimental import pallas as pl
from jax.experimental.pallas import tpu as pltpu
from jax.sharding import PartitionSpec as P

EPSILON = 1e-06
MESH = pl.DeviceIdType.MESH
BF16 = jnp.bfloat16
F32 = jnp.float32
HEAD_DIM = 72
LANES = 128
SLAB = 4
LOG2E = 1.4426950408889634
SCORE_SCALE = LOG2E / math.sqrt(HEAD_DIM)


def norm_rows(values, gain):
    mean = jnp.sum(values * values, axis=0, keepdims=True) * (1.0 / HEAD_DIM)
    return values * lax.rsqrt(mean + EPSILON) * gain


def fused_kernel(
    x_ref,
    residual_ref,
    proj_ref,
    weight_ref,
    gate_ref,
    shift_ref,
    scale_ref,
    spatial_qgain_ref,
    spatial_kgain_ref,
    temporal_qgain_ref,
    temporal_kgain_ref,
    out_ref,
    taken,
    residual,
    proj,
    weight,
    gains,
    wide,
    send,
    recv,
    queries,
    keys,
    values,
    scores,
    outgoing,
    attended,
    slabs,
    slab_recv,
    turned,
    result,
    slab_outgoing,
    slab_back,
    load_sem,
    take_sem,
    send_sem,
    recv_sem,
    back_send_sem,
    back_recv_sem,
    slab_send_sem,
    slab_recv_sem,
    slab_back_send_sem,
    slab_back_recv_sem,
    known_sem,
):
    me = lax.axis_index("pos")
    frame = lax.axis_index("frame")
    odd = lax.rem(me, 2)

    def take(s):
        j = lax.rem(me + 1 + s, 9)
        columns = pl.ds(pl.multiple_of(j * LANES, LANES), LANES)
        return pltpu.make_async_copy(
            x_ref.at[:, :, :, columns], taken.at[s], take_sem.at[s]
        )

    for s in range(9):
        take(s).start()
    barrier = pltpu.get_barrier_semaphore()
    for r in range(1, 8):
        pl.semaphore_signal(
            barrier, inc=1, device_id={"pos": lax.rem(me + r, 8)}, device_id_type=MESH
        )

    y, z, core = frame // 8, lax.rem(frame // 2, 4), lax.rem(frame, 2)

    def at(y, z, core):
        return (lax.rem(y, 4) * 4 + lax.rem(z, 4)) * 2 + lax.rem(core, 2)

    beside_core = (at(y, z, core + 1),)
    beside_y = (at(y + 1, z, core), at(y + 3, z, core))
    beside_z = (at(y, z + 1, core), at(y, z + 3, core))
    for neighbour in beside_core + beside_y + beside_z:
        pl.semaphore_signal(barrier, inc=1, device_id={"frame": neighbour}, device_id_type=MESH)
    rounds = (beside_core, beside_y, beside_z, beside_z)

    def tell(n):
        for neighbour in rounds[n]:
            pl.semaphore_signal(
                known_sem.at[n], inc=1, device_id={"frame": neighbour}, device_id_type=MESH
            )

    def hear(n):
        pl.semaphore_wait(known_sem.at[n], len(rounds[n]))

    loads = [
        pltpu.make_async_copy(source, target, load_sem.at[n])
        for n, (source, target) in enumerate(
            ((residual_ref, residual), (proj_ref, proj), (weight_ref, weight))
        )
    ]
    for load in loads:
        load.start()
    for n, gain_ref in enumerate(
        (spatial_qgain_ref, spatial_kgain_ref, temporal_qgain_ref, temporal_kgain_ref)
    ):
        column = jnp.broadcast_to(gain_ref[...], (LANES, HEAD_DIM)).T
        for m in range(3):
            gains[n, :, 128 * m : 128 * m + 128] = column

    swap = jnp.zeros((64, LANES), jnp.int32) + odd == 1

    def turn(s):
        j = lax.rem(me + 1 + s, 9)
        rows = pl.ds(pl.multiple_of(j * LANES, LANES), LANES)
        for t in range(3):
            first = taken[s, 0, t].astype(F32)
            second = taken[s, 1, t].astype(F32)
            low, high = first[128:], second[:64]
            block = jnp.concatenate(
                [first[:128], jnp.where(swap, high, low), jnp.where(swap, low, high), second[64:]],
                axis=0,
            )
            wide[t, rows, :] = block.T

    def pack(d, h):
        rows = pl.ds(pl.multiple_of(d * 144 + 72 * h, 8), HEAD_DIM)
        send[2 * d + h, 0] = norm_rows(wide[0, rows, :], gains[0]).astype(BF16)
        send[2 * d + h, 1] = norm_rows(wide[1, rows, :], gains[1]).astype(BF16)
        send[2 * d + h, 2] = wide[2, rows, :].astype(BF16)

    def exchange(stage, peer, r):
        h = 0 if stage == 0 else 1
        part = ((0, 3), (1, 2), (0, 1))[stage]
        return pltpu.make_async_remote_copy(
            src_ref=send.at[2 * peer + h, pl.ds(*part)],
            dst_ref=recv.at[h, r, pl.ds(*part)],
            send_sem=send_sem.at[stage, r],
            recv_sem=recv_sem.at[stage, r],
            device_id={"pos": peer},
            device_id_type=MESH,
        )

    take(0).wait()
    turn(0)
    take(1).wait()
    turn(1)
    pl.semaphore_wait(barrier, 12)
    tell(0)

    def feed(s, carry):
        @pl.when(s > 1)
        def _():
            take(s).wait()
            turn(s)

        j = lax.rem(me + 1 + s, 9)

        @pl.when(j >= 1)
        def _():
            peer = j - 1
            pack(peer, 0)
            exchange(0, peer, lax.rem(peer + 8 - me, 8)).start()

        return carry

    lax.fori_loop(1, 9, feed, 0)
    hear(0)
    tell(1)

    def feed_second(r, carry):
        peer = lax.rem(me + r, 8)
        pack(peer, 1)
        exchange(1, peer, r).start()
        return carry

    lax.fori_loop(1, 8, feed_second, 0)
    hear(1)
    tell(2)
    for r in range(1, 8):
        exchange(2, lax.rem(me + r, 8), r).start()
    for h in range(2):
        pack(me, h)
        recv[h, 0] = send[2 * me + h]
    for v in range(2):
        values[v, 72:80, :] = jnp.ones((8, 1536), BF16)

    lane = lax.broadcasted_iota(jnp.int32, (HEAD_DIM, LANES), 1)
    straight = (lane < 64) == ((jnp.zeros((HEAD_DIM, LANES), jnp.int32) + odd) == 0)

    def give_back(h, r):
        return pltpu.make_async_remote_copy(
            src_ref=outgoing.at[h, r],
            dst_ref=attended.at[2 * me + h],
            send_sem=back_send_sem.at[h, r],
            recv_sem=back_recv_sem.at[h, r],
            device_id={"pos": lax.rem(me + 8 - r, 8)},
            device_id_type=MESH,
        )

    def await_pair(stage, i):
        for r in (2 * i, 2 * i + 1):
            if r > 0:
                exchange(stage, lax.rem(me + r, 8), r).wait_recv()

    def spread(h, i, t):
        a, b = recv[h, 2 * i, t], recv[h, 2 * i + 1, t]
        amid, bmid = a[:, 128:256].astype(F32), b[:, 128:256].astype(F32)
        mids = (
            jnp.where(straight, amid, bmid).astype(BF16),
            jnp.where(straight, bmid, amid).astype(BF16),
        )
        for v in range(2):
            edge = slice(256 * v, 256 * v + 128)
            for n, piece in enumerate((a[:, edge], b[:, edge], mids[v])):
                place = slice(384 * i + 128 * n, 384 * i + 128 * n + 128)
                if t == 0:
                    queries[v, :, place] = piece
                elif t == 1:
                    keys[v, place, :] = piece.T
                else:
                    values[v, 0:72, place] = piece

    for h in range(2):
        for i in range(4):
            await_pair(h, i)
            spread(h, i, 1)
            spread(h, i, 2)
        hear(2 + h)
        if h == 0:
            tell(3)
        for g in range(2):
            for i in (2 * g, 2 * g + 1):
                if h == 1:
                    await_pair(2, i)
                spread(h, i, 0)
            results = []
            for v in range(2):
                block = queries[v, :, 768 * g : 768 * g + 768]
                top = None
                for c in range(6):
                    part = jnp.dot(
                        keys[v, 256 * c : 256 * c + 256, :], block, preferred_element_type=F32
                    )
                    scores[v, 256 * c : 256 * c + 256, :] = part
                    part_top = jnp.max(part.reshape(32, 8, 768), axis=0)
                    top = part_top if top is None else jnp.maximum(top, part_top)
                top = jnp.max(top, axis=0, keepdims=True) * SCORE_SCALE
                total = None
                for c in range(6):
                    expons = jnp.exp2(
                        scores[v, 256 * c : 256 * c + 256, :] * SCORE_SCALE - top
                    ).astype(BF16)
                    part = jnp.dot(
                        values[v, :, 256 * c : 256 * c + 256], expons, preferred_element_type=F32
                    )
                    total = part if total is None else total + part
                results.append(total[:72] / total[72:73])
            for i in (2 * g, 2 * g + 1):
                base = 384 * (i - 2 * g)
                mid0 = results[0][:, base + 256 : base + 384]
                mid1 = results[1][:, base + 256 : base + 384]
                for n in range(2):
                    r = 2 * i + n
                    edge = slice(base + 128 * n, base + 128 * n + 128)
                    if n == 0:
                        mid = jnp.where(straight, mid0, mid1)
                    else:
                        mid = jnp.where(straight, mid1, mid0)
                    pieces = (results[0][:, edge], mid, results[1][:, edge])
                    for m, piece in enumerate(pieces):
                        place = slice(128 * m, 128 * m + 128)
                        if r == 0:
                            attended[2 * me + h, :, place] = piece.astype(BF16)
                        else:
                            outgoing[h, r, :, place] = piece.astype(BF16)
                    if r > 0:
                        give_back(h, r).start()

    def arrived(h, r):
        return pltpu.make_async_remote_copy(
            src_ref=outgoing.at[h, r],
            dst_ref=attended.at[2 * lax.rem(me + r, 8) + h],
            send_sem=back_send_sem.at[h, r],
            recv_sem=back_recv_sem.at[h, r],
            device_id={"pos": lax.rem(me + r, 8)},
            device_id_type=MESH,
        )

    for load in loads:
        load.wait()
    for h in range(2):
        for r in range(1, 8):
            arrived(h, r).wait_recv()
    for n in range(16):
        wide[0, 72 * n : 72 * n + 72, :] = attended[n].astype(F32)
    swap_rows = jnp.zeros((LANES, 1152), jnp.int32) + odd == 1

    def give_slab(i, r):
        peer = lax.rem(frame + r, 32)
        return pltpu.make_async_remote_copy(
            src_ref=slabs.at[32 * i + peer],
            dst_ref=slab_recv.at[i, r],
            send_sem=slab_send_sem.at[i],
            recv_sem=slab_recv_sem.at[i],
            device_id={"frame": peer},
            device_id_type=MESH,
        )

    for tile in range(3):
        rows = wide[0, :, 128 * tile : 128 * tile + 128].T
        if tile == 1:
            rows = jnp.where(swap_rows, jnp.concatenate([rows[64:], rows[:64]], axis=0), rows)
        mixed = jnp.dot(rows.astype(BF16), proj[...], preferred_element_type=F32)
        for half in range(2):
            start = 128 * tile + 64 * half
            v, p = divmod(start, 192)
            updated = (
                residual[v, p : p + 64, :].astype(F32)
                + gate_ref[v : v + 1, :] * mixed[64 * half : 64 * half + 64]
            ).astype(BF16)
            widened = updated.astype(F32)
            centred = widened - jnp.mean(widened, axis=-1, keepdims=True)
            spread_of = jnp.mean(centred * centred, axis=-1, keepdims=True)
            scaled = centred * lax.rsqrt(spread_of + EPSILON) * (1.0 + scale_ref[v : v + 1, :])
            normed = (scaled + shift_ref[v : v + 1, :]).astype(BF16)
            slabs[start // SLAB : start // SLAB + 16] = normed.reshape(16, SLAB, 1152)

        def give(r, carry):
            give_slab(tile, r).start()
            return carry

        lax.fori_loop(1, 32, give, 0)
        slab_recv[tile, 0] = slabs[32 * tile + frame]

    def all_of(buffer, send_sem, recv_sem):
        return pltpu.make_async_remote_copy(
            src_ref=buffer,
            dst_ref=buffer,
            send_sem=send_sem,
            recv_sem=recv_sem,
            device_id={"frame": lax.rem(frame + 1, 32)},
            device_id_type=MESH,
        )

    row = lax.broadcasted_iota(jnp.int32, (LANES, LANES), 0)
    column = lax.broadcasted_iota(jnp.int32, (LANES, LANES), 1)
    same = lax.rem(row, SLAB) == lax.rem(column, SLAB)
    for i in range(3):
        all_of(
            slab_recv.at[i, pl.ds(1, 31)], slab_send_sem.at[i], slab_recv_sem.at[i]
        ).wait_recv()
        tokens = slab_recv[i].reshape(LANES, 1152)
        for t in range(3):
            projected = jnp.dot(
                tokens, weight[:, 1152 * t : 1152 * t + 1152], preferred_element_type=F32
            ).astype(BF16)
            turned[t] = projected.astype(F32).T
        for n in range(16):
            head = slice(72 * n, 72 * n + 72)
            query = norm_rows(turned[0, head, :], gains[2, :, 0:128]).astype(BF16)
            key = norm_rows(turned[1, head, :], gains[3, :, 0:128]).astype(BF16)
            score = lax.dot_general(
                key, query, (((0,), (0,)), ((), ())), preferred_element_type=F32
            )
            score = jnp.where(same, score * SCORE_SCALE, -1e30)
            expons = jnp.exp2(score - jnp.max(score, axis=0, keepdims=True))
            share = (expons / jnp.sum(expons, axis=0, keepdims=True)).astype(BF16)
            result[head, :] = jnp.dot(
                turned[2, head, :].astype(BF16), share, preferred_element_type=F32
            )
        slab_outgoing[i] = result[...].T.astype(BF16).reshape(32, SLAB, 1152)

        def return_slab(r, carry):
            pltpu.make_async_remote_copy(
                src_ref=slab_outgoing.at[i, r],
                dst_ref=slab_back.at[32 * i + frame],
                send_sem=slab_back_send_sem.at[i],
                recv_sem=slab_back_recv_sem.at[i],
                device_id={"frame": lax.rem(frame + 32 - r, 32)},
                device_id_type=MESH,
            ).start()
            return carry

        lax.fori_loop(1, 32, return_slab, 0)
        slab_back[32 * i + frame] = slab_outgoing[i, 0]
    for stage in range(3):
        for r in range(1, 8):
            exchange(stage, lax.rem(me + r, 8), r).wait_send()
    for h in range(2):
        for r in range(1, 8):
            give_back(h, r).wait_send()
    for i in range(3):
        all_of(
            slab_back.at[pl.ds(32 * i, 31)], slab_back_send_sem.at[i], slab_back_recv_sem.at[i]
        ).wait_recv()
        out_ref[128 * i : 128 * i + 128, :] = slab_back[32 * i : 32 * i + 32].reshape(128, 1152)
    for i in range(3):
        all_of(
            slab_recv.at[i, pl.ds(1, 31)], slab_send_sem.at[i], slab_recv_sem.at[i]
        ).wait_send()
        all_of(
            slab_back.at[pl.ds(32 * i, 31)], slab_back_send_sem.at[i], slab_back_recv_sem.at[i]
        ).wait_send()


def per_device(
    spatial_qkv,
    residual,
    spatial_gate,
    spatial_proj,
    spatial_qgain,
    spatial_kgain,
    temporal_shift,
    temporal_scale,
    temporal_qkv,
    temporal_qgain,
    temporal_kgain,
):
    vmem = pl.BlockSpec(memory_space=pltpu.VMEM)
    anywhere = pl.BlockSpec(memory_space=pl.ANY)
    dma = pltpu.SemaphoreType.DMA
    split = jnp.transpose(spatial_qkv, (0, 1, 3, 2, 4)).reshape(2, 3, 192, 1152)
    result = pl.pallas_call(
        fused_kernel,
        out_shape=jax.ShapeDtypeStruct((384, 1152), BF16),
        in_specs=[anywhere] * 4 + [vmem] * 7,
        out_specs=vmem,
        scratch_shapes=[
            pltpu.VMEM((9, 2, 3, 192, LANES), BF16),
            pltpu.VMEM((2, 192, 1152), BF16),
            pltpu.VMEM((1152, 1152), BF16),
            pltpu.VMEM((1152, 3456), BF16),
            pltpu.VMEM((4, 72, 384), F32),
            pltpu.VMEM((3, 1152, 384), F32),
            pltpu.VMEM((16, 3, 72, 384), BF16),
            pltpu.VMEM((2, 8, 3, 72, 384), BF16),
            pltpu.VMEM((2, 72, 1536), BF16),
            pltpu.VMEM((2, 1536, 72), BF16),
            pltpu.VMEM((2, 80, 1536), BF16),
            pltpu.VMEM((2, 1536, 768), F32),
            pltpu.VMEM((2, 8, 72, 384), BF16),
            pltpu.VMEM((16, 72, 384), BF16),
            pltpu.VMEM((96, SLAB, 1152), BF16),
            pltpu.VMEM((3, 32, SLAB, 1152), BF16),
            pltpu.VMEM((3, 1152, LANES), F32),
            pltpu.VMEM((1152, LANES), F32),
            pltpu.VMEM((3, 32, SLAB, 1152), BF16),
            pltpu.VMEM((96, SLAB, 1152), BF16),
            dma((3,)),
            dma((9,)),
            dma((3, 8)),
            dma((3, 8)),
            dma((2, 8)),
            dma((2, 8)),
            dma((3,)),
            dma((3,)),
            dma((3,)),
            dma((3,)),
            pltpu.SemaphoreType.REGULAR((4,)),
        ],
        compiler_params=pltpu.CompilerParams(
            collective_id=0, has_side_effects=True, vmem_limit_bytes=62 * 1024 * 1024
        ),
        name="fused",
    )(
        split,
        residual.reshape(2, 192, 1152),
        spatial_proj,
        temporal_qkv,
        spatial_gate,
        temporal_shift,
        temporal_scale,
        spatial_qgain.reshape(1, 72),
        spatial_kgain.reshape(1, 72),
        temporal_qgain.reshape(1, 72),
        temporal_kgain.reshape(1, 72),
    )
    return result.reshape(2, 1, 192, 1152)


def solution(mesh):
    return jax.shard_map(
        per_device,
        mesh=mesh,
        in_specs=(
            P(None, "frame", "pos", None, None),
            P(None, "frame", "pos", None),
            P(),
            P(),
            P(),
            P(),
            P(),
            P(),
            P(),
            P(),
            P(),
        ),
        out_specs=P(None, "frame", "pos", None),
        check_vma=False,
    )
```

```python
import math

import jax
import jax.numpy as jnp
from jax import lax
from jax.experimental import pallas as pl
from jax.experimental.pallas import tpu as pltpu
from jax.sharding import PartitionSpec as P

EPSILON = 1e-06
MESH = pl.DeviceIdType.MESH
BF16 = jnp.bfloat16
F32 = jnp.float32
HEAD_DIM = 72
LANES = 128
SLAB = 4
LOG2E = 1.4426950408889634
SCORE_SCALE = LOG2E / math.sqrt(HEAD_DIM)


def norm_rows(values, gain):
    mean = jnp.sum(values * values, axis=0, keepdims=True) * (1.0 / HEAD_DIM)
    return values * lax.rsqrt(mean + EPSILON) * gain


def fused_kernel(
    x_ref,
    residual_ref,
    proj_ref,
    weight_ref,
    gate_ref,
    shift_ref,
    scale_ref,
    spatial_qgain_ref,
    spatial_kgain_ref,
    temporal_qgain_ref,
    temporal_kgain_ref,
    out_ref,
    taken,
    residual,
    proj,
    weight,
    gains,
    wide,
    send,
    recv,
    queries,
    keys,
    values,
    scores,
    outgoing,
    attended,
    slabs,
    slab_recv,
    turned,
    result,
    slab_outgoing,
    slab_back,
    load_sem,
    take_sem,
    send_sem,
    recv_sem,
    back_send_sem,
    back_recv_sem,
    slab_send_sem,
    slab_recv_sem,
    slab_back_send_sem,
    slab_back_recv_sem,
    known_sem,
):
    me = lax.axis_index("pos")
    frame = lax.axis_index("frame")
    odd = lax.rem(me, 2)

    def take(s):
        j = lax.rem(me + 1 + s, 9)
        columns = pl.ds(pl.multiple_of(j * LANES, LANES), LANES)
        return pltpu.make_async_copy(
            x_ref.at[:, :, :, columns], taken.at[s], take_sem.at[s]
        )

    for s in range(9):
        take(s).start()
    barrier = pltpu.get_barrier_semaphore()
    for r in range(1, 8):
        pl.semaphore_signal(
            barrier, inc=1, device_id={"pos": lax.rem(me + r, 8)}, device_id_type=MESH
        )

    y, z, core = frame // 8, lax.rem(frame // 2, 4), lax.rem(frame, 2)

    def at(y, z, core):
        return (lax.rem(y, 4) * 4 + lax.rem(z, 4)) * 2 + lax.rem(core, 2)

    beside_core = (at(y, z, core + 1),)
    beside_y = (at(y + 1, z, core), at(y + 3, z, core))
    beside_z = (at(y, z + 1, core), at(y, z + 3, core))
    for neighbour in beside_core + beside_y + beside_z:
        pl.semaphore_signal(barrier, inc=1, device_id={"frame": neighbour}, device_id_type=MESH)
    rounds = (beside_core, beside_y, beside_z, beside_z)

    def tell(n):
        for neighbour in rounds[n]:
            pl.semaphore_signal(
                known_sem.at[n], inc=1, device_id={"frame": neighbour}, device_id_type=MESH
            )

    def hear(n):
        pl.semaphore_wait(known_sem.at[n], len(rounds[n]))

    loads = [
        pltpu.make_async_copy(source, target, load_sem.at[n])
        for n, (source, target) in enumerate(
            ((residual_ref, residual), (proj_ref, proj), (weight_ref, weight))
        )
    ]
    for load in loads:
        load.start()
    for n, gain_ref in enumerate(
        (spatial_qgain_ref, spatial_kgain_ref, temporal_qgain_ref, temporal_kgain_ref)
    ):
        column = jnp.broadcast_to(gain_ref[...], (LANES, HEAD_DIM)).T
        for m in range(3):
            gains[n, :, 128 * m : 128 * m + 128] = column

    swap = jnp.zeros((64, LANES), jnp.int32) + odd == 1

    def turn(s):
        j = lax.rem(me + 1 + s, 9)
        rows = pl.ds(pl.multiple_of(j * LANES, LANES), LANES)
        for t in range(3):
            first = taken[s, 0, t].astype(F32)
            second = taken[s, 1, t].astype(F32)
            low, high = first[128:], second[:64]
            block = jnp.concatenate(
                [first[:128], jnp.where(swap, high, low), jnp.where(swap, low, high), second[64:]],
                axis=0,
            )
            wide[t, rows, :] = block.T

    def pack(d, h):
        rows = pl.ds(pl.multiple_of(d * 144 + 72 * h, 8), HEAD_DIM)
        send[2 * d + h, 0] = norm_rows(wide[0, rows, :], gains[0]).astype(BF16)
        send[2 * d + h, 1] = norm_rows(wide[1, rows, :], gains[1]).astype(BF16)
        send[2 * d + h, 2] = wide[2, rows, :].astype(BF16)

    def exchange(stage, peer, r):
        h = 0 if stage == 0 else 1
        part = ((0, 3), (1, 2), (0, 1))[stage]
        return pltpu.make_async_remote_copy(
            src_ref=send.at[2 * peer + h, pl.ds(*part)],
            dst_ref=recv.at[h, r, pl.ds(*part)],
            send_sem=send_sem.at[stage, r],
            recv_sem=recv_sem.at[stage, r],
            device_id={"pos": peer},
            device_id_type=MESH,
        )

    take(0).wait()
    turn(0)
    take(1).wait()
    turn(1)
    pl.semaphore_wait(barrier, 12)
    tell(0)

    def feed(s, carry):
        @pl.when(s > 1)
        def _():
            take(s).wait()
            turn(s)

        j = lax.rem(me + 1 + s, 9)

        @pl.when(j >= 1)
        def _():
            peer = j - 1
            pack(peer, 0)
            exchange(0, peer, lax.rem(peer + 8 - me, 8)).start()

        return carry

    lax.fori_loop(1, 9, feed, 0)
    hear(0)
    tell(1)

    def feed_second(r, carry):
        peer = lax.rem(me + r, 8)
        pack(peer, 1)
        exchange(1, peer, r).start()
        return carry

    lax.fori_loop(1, 8, feed_second, 0)
    hear(1)
    tell(2)
    for r in range(1, 8):
        exchange(2, lax.rem(me + r, 8), r).start()
    for h in range(2):
        pack(me, h)
        recv[h, 0] = send[2 * me + h]
    for v in range(2):
        values[v, 72:80, :] = jnp.ones((8, 1536), BF16)

    lane = lax.broadcasted_iota(jnp.int32, (HEAD_DIM, LANES), 1)
    straight = (lane < 64) == ((jnp.zeros((HEAD_DIM, LANES), jnp.int32) + odd) == 0)

    def give_back(h, r, tile):
        span = pl.ds(128 * tile, 128)
        return pltpu.make_async_remote_copy(
            src_ref=outgoing.at[h, r, :, span],
            dst_ref=attended.at[2 * me + h, :, span],
            send_sem=back_send_sem.at[h, r, tile],
            recv_sem=back_recv_sem.at[h, r, tile],
            device_id={"pos": lax.rem(me + 8 - r, 8)},
            device_id_type=MESH,
        )

    def await_pair(stage, i):
        for r in (2 * i, 2 * i + 1):
            if r > 0:
                exchange(stage, lax.rem(me + r, 8), r).wait_recv()

    def spread(h, i, t):
        a, b = recv[h, 2 * i, t], recv[h, 2 * i + 1, t]
        amid, bmid = a[:, 128:256].astype(F32), b[:, 128:256].astype(F32)
        mids = (
            jnp.where(straight, amid, bmid).astype(BF16),
            jnp.where(straight, bmid, amid).astype(BF16),
        )
        for v in range(2):
            edge = slice(256 * v, 256 * v + 128)
            for n, piece in enumerate((a[:, edge], b[:, edge], mids[v])):
                place = slice(384 * i + 128 * n, 384 * i + 128 * n + 128)
                if t == 0:
                    queries[v, :, place] = piece
                elif t == 1:
                    keys[v, place, :] = piece.T
                else:
                    values[v, 0:72, place] = piece

    for h in range(2):
        for i in range(4):
            await_pair(h, i)
            spread(h, i, 1)
            spread(h, i, 2)
        hear(2 + h)
        if h == 0:
            tell(3)
        for g in range(2):
            for i in (2 * g, 2 * g + 1):
                if h == 1:
                    await_pair(2, i)
                spread(h, i, 0)
            results = []
            for v in range(2):
                block = queries[v, :, 768 * g : 768 * g + 768]
                top = None
                for c in range(6):
                    part = jnp.dot(
                        keys[v, 256 * c : 256 * c + 256, :], block, preferred_element_type=F32
                    )
                    scores[v, 256 * c : 256 * c + 256, :] = part
                    part_top = jnp.max(part.reshape(32, 8, 768), axis=0)
                    top = part_top if top is None else jnp.maximum(top, part_top)
                top = jnp.max(top, axis=0, keepdims=True) * SCORE_SCALE
                total = None
                for c in range(6):
                    expons = jnp.exp2(
                        scores[v, 256 * c : 256 * c + 256, :] * SCORE_SCALE - top
                    ).astype(BF16)
                    part = jnp.dot(
                        values[v, :, 256 * c : 256 * c + 256], expons, preferred_element_type=F32
                    )
                    total = part if total is None else total + part
                results.append(total[:72] / total[72:73])
            for i in (2 * g, 2 * g + 1):
                base = 384 * (i - 2 * g)
                mid0 = results[0][:, base + 256 : base + 384]
                mid1 = results[1][:, base + 256 : base + 384]
                for n in range(2):
                    r = 2 * i + n
                    edge = slice(base + 128 * n, base + 128 * n + 128)
                    if n == 0:
                        mid = jnp.where(straight, mid0, mid1)
                    else:
                        mid = jnp.where(straight, mid1, mid0)
                    pieces = (results[0][:, edge], mid, results[1][:, edge])
                    for m, piece in enumerate(pieces):
                        place = slice(128 * m, 128 * m + 128)
                        if r == 0:
                            attended[2 * me + h, :, place] = piece.astype(BF16)
                        else:
                            outgoing[h, r, :, place] = piece.astype(BF16)
            for tile in range(3):
                for r in range(max(4 * g, 1), 4 * g + 4):
                    give_back(h, r, tile).start()

    def arrived(h, r, tile):
        span = pl.ds(128 * tile, 128)
        return pltpu.make_async_remote_copy(
            src_ref=outgoing.at[h, r, :, span],
            dst_ref=attended.at[2 * lax.rem(me + r, 8) + h, :, span],
            send_sem=back_send_sem.at[h, r, tile],
            recv_sem=back_recv_sem.at[h, r, tile],
            device_id={"pos": lax.rem(me + r, 8)},
            device_id_type=MESH,
        )

    for load in loads:
        load.wait()
    swap_rows = jnp.zeros((LANES, 1152), jnp.int32) + odd == 1

    def give_slab(i, r):
        peer = lax.rem(frame + r, 32)
        return pltpu.make_async_remote_copy(
            src_ref=slabs.at[32 * i + peer],
            dst_ref=slab_recv.at[i, r],
            send_sem=slab_send_sem.at[i],
            recv_sem=slab_recv_sem.at[i],
            device_id={"frame": peer},
            device_id_type=MESH,
        )

    for tile in range(3):
        span = slice(128 * tile, 128 * tile + 128)
        for h in range(2):
            for r in range(1, 8):
                arrived(h, r, tile).wait_recv()
        for n in range(16):
            wide[0, 72 * n : 72 * n + 72, span] = attended[n, :, span].astype(F32)
        rows = wide[0, :, span].T
        if tile == 1:
            rows = jnp.where(swap_rows, jnp.concatenate([rows[64:], rows[:64]], axis=0), rows)
        mixed = jnp.dot(rows.astype(BF16), proj[...], preferred_element_type=F32)
        for half in range(2):
            start = 128 * tile + 64 * half
            v, p = divmod(start, 192)
            updated = (
                residual[v, p : p + 64, :].astype(F32)
                + gate_ref[v : v + 1, :] * mixed[64 * half : 64 * half + 64]
            ).astype(BF16)
            widened = updated.astype(F32)
            centred = widened - jnp.mean(widened, axis=-1, keepdims=True)
            spread_of = jnp.mean(centred * centred, axis=-1, keepdims=True)
            scaled = centred * lax.rsqrt(spread_of + EPSILON) * (1.0 + scale_ref[v : v + 1, :])
            normed = (scaled + shift_ref[v : v + 1, :]).astype(BF16)
            slabs[start // SLAB : start // SLAB + 16] = normed.reshape(16, SLAB, 1152)

        def give(r, carry):
            give_slab(tile, r).start()
            return carry

        lax.fori_loop(1, 32, give, 0)
        slab_recv[tile, 0] = slabs[32 * tile + frame]

    def all_of(buffer, send_sem, recv_sem):
        return pltpu.make_async_remote_copy(
            src_ref=buffer,
            dst_ref=buffer,
            send_sem=send_sem,
            recv_sem=recv_sem,
            device_id={"frame": lax.rem(frame + 1, 32)},
            device_id_type=MESH,
        )

    row = lax.broadcasted_iota(jnp.int32, (LANES, LANES), 0)
    column = lax.broadcasted_iota(jnp.int32, (LANES, LANES), 1)
    same = lax.rem(row, SLAB) == lax.rem(column, SLAB)
    for i in range(3):
        all_of(
            slab_recv.at[i, pl.ds(1, 31)], slab_send_sem.at[i], slab_recv_sem.at[i]
        ).wait_recv()
        tokens = slab_recv[i].reshape(LANES, 1152)
        for t in range(3):
            projected = jnp.dot(
                tokens, weight[:, 1152 * t : 1152 * t + 1152], preferred_element_type=F32
            ).astype(BF16)
            turned[t] = projected.astype(F32).T
        for n in range(16):
            head = slice(72 * n, 72 * n + 72)
            query = norm_rows(turned[0, head, :], gains[2, :, 0:128]).astype(BF16)
            key = norm_rows(turned[1, head, :], gains[3, :, 0:128]).astype(BF16)
            score = lax.dot_general(
                key, query, (((0,), (0,)), ((), ())), preferred_element_type=F32
            )
            score = jnp.where(same, score * SCORE_SCALE, -1e30)
            expons = jnp.exp2(score - jnp.max(score, axis=0, keepdims=True))
            share = (expons / jnp.sum(expons, axis=0, keepdims=True)).astype(BF16)
            result[head, :] = jnp.dot(
                turned[2, head, :].astype(BF16), share, preferred_element_type=F32
            )
        slab_outgoing[i] = result[...].T.astype(BF16).reshape(32, SLAB, 1152)

        def return_slab(r, carry):
            pltpu.make_async_remote_copy(
                src_ref=slab_outgoing.at[i, r],
                dst_ref=slab_back.at[32 * i + frame],
                send_sem=slab_back_send_sem.at[i],
                recv_sem=slab_back_recv_sem.at[i],
                device_id={"frame": lax.rem(frame + 32 - r, 32)},
                device_id_type=MESH,
            ).start()
            return carry

        lax.fori_loop(1, 32, return_slab, 0)
        slab_back[32 * i + frame] = slab_outgoing[i, 0]
    for stage in range(3):
        for r in range(1, 8):
            exchange(stage, lax.rem(me + r, 8), r).wait_send()
    for h in range(2):
        for r in range(1, 8):
            for tile in range(3):
                give_back(h, r, tile).wait_send()
    for i in range(3):
        all_of(
            slab_back.at[pl.ds(32 * i, 31)], slab_back_send_sem.at[i], slab_back_recv_sem.at[i]
        ).wait_recv()
        out_ref[128 * i : 128 * i + 128, :] = slab_back[32 * i : 32 * i + 32].reshape(128, 1152)
    for i in range(3):
        all_of(
            slab_recv.at[i, pl.ds(1, 31)], slab_send_sem.at[i], slab_recv_sem.at[i]
        ).wait_send()
        all_of(
            slab_back.at[pl.ds(32 * i, 31)], slab_back_send_sem.at[i], slab_back_recv_sem.at[i]
        ).wait_send()


def per_device(
    spatial_qkv,
    residual,
    spatial_gate,
    spatial_proj,
    spatial_qgain,
    spatial_kgain,
    temporal_shift,
    temporal_scale,
    temporal_qkv,
    temporal_qgain,
    temporal_kgain,
):
    vmem = pl.BlockSpec(memory_space=pltpu.VMEM)
    anywhere = pl.BlockSpec(memory_space=pl.ANY)
    dma = pltpu.SemaphoreType.DMA
    split = jnp.transpose(spatial_qkv, (0, 1, 3, 2, 4)).reshape(2, 3, 192, 1152)
    result = pl.pallas_call(
        fused_kernel,
        out_shape=jax.ShapeDtypeStruct((384, 1152), BF16),
        in_specs=[anywhere] * 4 + [vmem] * 7,
        out_specs=vmem,
        scratch_shapes=[
            pltpu.VMEM((9, 2, 3, 192, LANES), BF16),
            pltpu.VMEM((2, 192, 1152), BF16),
            pltpu.VMEM((1152, 1152), BF16),
            pltpu.VMEM((1152, 3456), BF16),
            pltpu.VMEM((4, 72, 384), F32),
            pltpu.VMEM((3, 1152, 384), F32),
            pltpu.VMEM((16, 3, 72, 384), BF16),
            pltpu.VMEM((2, 8, 3, 72, 384), BF16),
            pltpu.VMEM((2, 72, 1536), BF16),
            pltpu.VMEM((2, 1536, 72), BF16),
            pltpu.VMEM((2, 80, 1536), BF16),
            pltpu.VMEM((2, 1536, 768), F32),
            pltpu.VMEM((2, 8, 72, 384), BF16),
            pltpu.VMEM((16, 72, 384), BF16),
            pltpu.VMEM((96, SLAB, 1152), BF16),
            pltpu.VMEM((3, 32, SLAB, 1152), BF16),
            pltpu.VMEM((3, 1152, LANES), F32),
            pltpu.VMEM((1152, LANES), F32),
            pltpu.VMEM((3, 32, SLAB, 1152), BF16),
            pltpu.VMEM((96, SLAB, 1152), BF16),
            dma((3,)),
            dma((9,)),
            dma((3, 8)),
            dma((3, 8)),
            dma((2, 8, 3)),
            dma((2, 8, 3)),
            dma((3,)),
            dma((3,)),
            dma((3,)),
            dma((3,)),
            pltpu.SemaphoreType.REGULAR((4,)),
        ],
        compiler_params=pltpu.CompilerParams(
            collective_id=0, has_side_effects=True, vmem_limit_bytes=62 * 1024 * 1024
        ),
        name="fused",
    )(
        split,
        residual.reshape(2, 192, 1152),
        spatial_proj,
        temporal_qkv,
        spatial_gate,
        temporal_shift,
        temporal_scale,
        spatial_qgain.reshape(1, 72),
        spatial_kgain.reshape(1, 72),
        temporal_qgain.reshape(1, 72),
        temporal_kgain.reshape(1, 72),
    )
    return result.reshape(2, 1, 192, 1152)


def solution(mesh):
    return jax.shard_map(
        per_device,
        mesh=mesh,
        in_specs=(
            P(None, "frame", "pos", None, None),
            P(None, "frame", "pos", None),
            P(),
            P(),
            P(),
            P(),
            P(),
            P(),
            P(),
            P(),
            P(),
        ),
        out_specs=P(None, "frame", "pos", None),
        check_vma=False,
    )
```

```python
import math

import jax
import jax.numpy as jnp
from jax import lax
from jax.experimental import pallas as pl
from jax.experimental.pallas import tpu as pltpu
from jax.sharding import PartitionSpec as P

EPSILON = 1e-06
MESH = pl.DeviceIdType.MESH
BF16 = jnp.bfloat16
F32 = jnp.float32
HEAD_DIM = 72
LANES = 128
SLAB = 4
LOG2E = 1.4426950408889634
SCORE_SCALE = LOG2E / math.sqrt(HEAD_DIM)


def norm_rows(values, gain):
    mean = jnp.sum(values * values, axis=0, keepdims=True) * (1.0 / HEAD_DIM)
    return values * lax.rsqrt(mean + EPSILON) * gain


def fused_kernel(
    x_ref,
    residual_ref,
    proj_ref,
    weight_ref,
    gate_ref,
    shift_ref,
    scale_ref,
    spatial_qgain_ref,
    spatial_kgain_ref,
    temporal_qgain_ref,
    temporal_kgain_ref,
    out_ref,
    taken,
    residual,
    proj,
    weight,
    gains,
    wide,
    send,
    recv,
    queries,
    keys,
    values,
    scores,
    outgoing,
    attended,
    slabs,
    slab_recv,
    turned,
    result,
    slab_outgoing,
    slab_back,
    load_sem,
    take_sem,
    send_sem,
    recv_sem,
    back_send_sem,
    back_recv_sem,
    slab_send_sem,
    slab_recv_sem,
    slab_back_send_sem,
    slab_back_recv_sem,
    known_sem,
    staged,
    store_sem,
):
    me = lax.axis_index("pos")
    frame = lax.axis_index("frame")
    odd = lax.rem(me, 2)

    def take(s):
        j = lax.rem(me + 1 + s, 9)
        columns = pl.ds(pl.multiple_of(j * LANES, LANES), LANES)
        return pltpu.make_async_copy(
            x_ref.at[:, :, :, columns], taken.at[s], take_sem.at[s]
        )

    for s in range(9):
        take(s).start()
    barrier = pltpu.get_barrier_semaphore()
    for r in range(1, 8):
        pl.semaphore_signal(
            barrier, inc=1, device_id={"pos": lax.rem(me + r, 8)}, device_id_type=MESH
        )

    y, z, core = frame // 8, lax.rem(frame // 2, 4), lax.rem(frame, 2)

    def at(y, z, core):
        return (lax.rem(y, 4) * 4 + lax.rem(z, 4)) * 2 + lax.rem(core, 2)

    beside_core = (at(y, z, core + 1),)
    beside_y = (at(y + 1, z, core), at(y + 3, z, core))
    beside_z = (at(y, z + 1, core), at(y, z + 3, core))
    for neighbour in beside_core + beside_y + beside_z:
        pl.semaphore_signal(barrier, inc=1, device_id={"frame": neighbour}, device_id_type=MESH)
    rounds = (beside_core, beside_y, beside_z, beside_z)

    def tell(n):
        for neighbour in rounds[n]:
            pl.semaphore_signal(
                known_sem.at[n], inc=1, device_id={"frame": neighbour}, device_id_type=MESH
            )

    def hear(n):
        pl.semaphore_wait(known_sem.at[n], len(rounds[n]))

    loads = [
        pltpu.make_async_copy(source, target, load_sem.at[n])
        for n, (source, target) in enumerate(
            ((residual_ref, residual), (proj_ref, proj), (weight_ref, weight))
        )
    ]
    for load in loads:
        load.start()
    for n, gain_ref in enumerate(
        (spatial_qgain_ref, spatial_kgain_ref, temporal_qgain_ref, temporal_kgain_ref)
    ):
        column = jnp.broadcast_to(gain_ref[...], (LANES, HEAD_DIM)).T
        for m in range(3):
            gains[n, :, 128 * m : 128 * m + 128] = column

    swap = jnp.zeros((64, LANES), jnp.int32) + odd == 1

    def turn(s):
        j = lax.rem(me + 1 + s, 9)
        rows = pl.ds(pl.multiple_of(j * LANES, LANES), LANES)
        for t in range(3):
            first = taken[s, 0, t].astype(F32)
            second = taken[s, 1, t].astype(F32)
            low, high = first[128:], second[:64]
            block = jnp.concatenate(
                [first[:128], jnp.where(swap, high, low), jnp.where(swap, low, high), second[64:]],
                axis=0,
            )
            wide[t, rows, :] = block.T

    def pack(d, h):
        rows = pl.ds(pl.multiple_of(d * 144 + 72 * h, 8), HEAD_DIM)
        send[2 * d + h, 0] = norm_rows(wide[0, rows, :], gains[0]).astype(BF16)
        send[2 * d + h, 1] = norm_rows(wide[1, rows, :], gains[1]).astype(BF16)
        send[2 * d + h, 2] = wide[2, rows, :].astype(BF16)

    def exchange(stage, peer, r):
        h = 0 if stage == 0 else 1
        part = ((0, 3), (1, 2), (0, 1))[stage]
        return pltpu.make_async_remote_copy(
            src_ref=send.at[2 * peer + h, pl.ds(*part)],
            dst_ref=recv.at[h, r, pl.ds(*part)],
            send_sem=send_sem.at[stage, r],
            recv_sem=recv_sem.at[stage, r],
            device_id={"pos": peer},
            device_id_type=MESH,
        )

    take(0).wait()
    turn(0)
    take(1).wait()
    turn(1)
    pl.semaphore_wait(barrier, 12)
    tell(0)

    def feed(s, carry):
        @pl.when(s > 1)
        def _():
            take(s).wait()
            turn(s)

        j = lax.rem(me + 1 + s, 9)

        @pl.when(j >= 1)
        def _():
            peer = j - 1
            pack(peer, 0)
            exchange(0, peer, lax.rem(peer + 8 - me, 8)).start()

        return carry

    lax.fori_loop(1, 9, feed, 0)
    hear(0)
    tell(1)

    def feed_second(r, carry):
        peer = lax.rem(me + r, 8)
        pack(peer, 1)
        exchange(1, peer, r).start()
        return carry

    lax.fori_loop(1, 8, feed_second, 0)
    hear(1)
    tell(2)
    for r in range(1, 8):
        exchange(2, lax.rem(me + r, 8), r).start()
    for h in range(2):
        pack(me, h)
        recv[h, 0] = send[2 * me + h]
    for v in range(2):
        values[v, 72:80, :] = jnp.ones((8, 1536), BF16)

    lane = lax.broadcasted_iota(jnp.int32, (HEAD_DIM, LANES), 1)
    straight = (lane < 64) == ((jnp.zeros((HEAD_DIM, LANES), jnp.int32) + odd) == 0)

    def give_back(h, r, tile):
        span = pl.ds(128 * tile, 128)
        return pltpu.make_async_remote_copy(
            src_ref=outgoing.at[h, r, :, span],
            dst_ref=attended.at[2 * me + h, :, span],
            send_sem=back_send_sem.at[h, r, tile],
            recv_sem=back_recv_sem.at[h, r, tile],
            device_id={"pos": lax.rem(me + 8 - r, 8)},
            device_id_type=MESH,
        )

    def await_pair(stage, i):
        for r in (2 * i, 2 * i + 1):
            if r > 0:
                exchange(stage, lax.rem(me + r, 8), r).wait_recv()

    def spread(h, i, t):
        a, b = recv[h, 2 * i, t], recv[h, 2 * i + 1, t]
        amid, bmid = a[:, 128:256].astype(F32), b[:, 128:256].astype(F32)
        mids = (
            jnp.where(straight, amid, bmid).astype(BF16),
            jnp.where(straight, bmid, amid).astype(BF16),
        )
        for v in range(2):
            edge = slice(256 * v, 256 * v + 128)
            for n, piece in enumerate((a[:, edge], b[:, edge], mids[v])):
                place = slice(384 * i + 128 * n, 384 * i + 128 * n + 128)
                if t == 0:
                    queries[v, :, place] = piece
                elif t == 1:
                    keys[v, place, :] = piece.T
                else:
                    values[v, 0:72, place] = piece

    for h in range(2):
        for i in range(4):
            await_pair(h, i)
            spread(h, i, 1)
            spread(h, i, 2)
        hear(2 + h)
        if h == 0:
            tell(3)
        for g in range(2):
            for i in (2 * g, 2 * g + 1):
                if h == 1:
                    await_pair(2, i)
                spread(h, i, 0)
            results = []
            for v in range(2):
                block = queries[v, :, 768 * g : 768 * g + 768]
                top = None
                for c in range(6):
                    part = jnp.dot(
                        keys[v, 256 * c : 256 * c + 256, :], block, preferred_element_type=F32
                    )
                    scores[v, 256 * c : 256 * c + 256, :] = part
                    part_top = jnp.max(part.reshape(32, 8, 768), axis=0)
                    top = part_top if top is None else jnp.maximum(top, part_top)
                top = jnp.max(top, axis=0, keepdims=True) * SCORE_SCALE
                total = None
                for c in range(6):
                    expons = jnp.exp2(
                        scores[v, 256 * c : 256 * c + 256, :] * SCORE_SCALE - top
                    ).astype(BF16)
                    part = jnp.dot(
                        values[v, :, 256 * c : 256 * c + 256], expons, preferred_element_type=F32
                    )
                    total = part if total is None else total + part
                results.append(total[:72] / total[72:73])
            for i in (2 * g, 2 * g + 1):
                base = 384 * (i - 2 * g)
                mid0 = results[0][:, base + 256 : base + 384]
                mid1 = results[1][:, base + 256 : base + 384]
                for n in range(2):
                    r = 2 * i + n
                    edge = slice(base + 128 * n, base + 128 * n + 128)
                    if n == 0:
                        mid = jnp.where(straight, mid0, mid1)
                    else:
                        mid = jnp.where(straight, mid1, mid0)
                    pieces = (results[0][:, edge], mid, results[1][:, edge])
                    for m, piece in enumerate(pieces):
                        place = slice(128 * m, 128 * m + 128)
                        if r == 0:
                            attended[2 * me + h, :, place] = piece.astype(BF16)
                        else:
                            outgoing[h, r, :, place] = piece.astype(BF16)
            for tile in range(3):
                for r in range(max(4 * g, 1), 4 * g + 4):
                    give_back(h, r, tile).start()

    def arrived(h, r, tile):
        span = pl.ds(128 * tile, 128)
        return pltpu.make_async_remote_copy(
            src_ref=outgoing.at[h, r, :, span],
            dst_ref=attended.at[2 * lax.rem(me + r, 8) + h, :, span],
            send_sem=back_send_sem.at[h, r, tile],
            recv_sem=back_recv_sem.at[h, r, tile],
            device_id={"pos": lax.rem(me + r, 8)},
            device_id_type=MESH,
        )

    for load in loads:
        load.wait()
    swap_rows = jnp.zeros((LANES, 1152), jnp.int32) + odd == 1

    def give_slab(i, r):
        peer = lax.rem(frame + r, 32)
        return pltpu.make_async_remote_copy(
            src_ref=slabs.at[32 * i + peer],
            dst_ref=slab_recv.at[i, r],
            send_sem=slab_send_sem.at[i],
            recv_sem=slab_recv_sem.at[i],
            device_id={"frame": peer},
            device_id_type=MESH,
        )

    for tile in range(3):
        span = slice(128 * tile, 128 * tile + 128)
        for h in range(2):
            for r in range(1, 8):
                arrived(h, r, tile).wait_recv()
        for n in range(16):
            wide[0, 72 * n : 72 * n + 72, span] = attended[n, :, span].astype(F32)
        rows = wide[0, :, span].T
        if tile == 1:
            rows = jnp.where(swap_rows, jnp.concatenate([rows[64:], rows[:64]], axis=0), rows)
        mixed = jnp.dot(rows.astype(BF16), proj[...], preferred_element_type=F32)
        for half in range(2):
            start = 128 * tile + 64 * half
            v, p = divmod(start, 192)
            updated = (
                residual[v, p : p + 64, :].astype(F32)
                + gate_ref[v : v + 1, :] * mixed[64 * half : 64 * half + 64]
            ).astype(BF16)
            widened = updated.astype(F32)
            centred = widened - jnp.mean(widened, axis=-1, keepdims=True)
            spread_of = jnp.mean(centred * centred, axis=-1, keepdims=True)
            scaled = centred * lax.rsqrt(spread_of + EPSILON) * (1.0 + scale_ref[v : v + 1, :])
            normed = (scaled + shift_ref[v : v + 1, :]).astype(BF16)
            slabs[start // SLAB : start // SLAB + 16] = normed.reshape(16, SLAB, 1152)

        def give(r, carry):
            give_slab(tile, r).start()
            return carry

        lax.fori_loop(1, 32, give, 0)
        slab_recv[tile, 0] = slabs[32 * tile + frame]

    def all_of(buffer, send_sem, recv_sem):
        return pltpu.make_async_remote_copy(
            src_ref=buffer,
            dst_ref=buffer,
            send_sem=send_sem,
            recv_sem=recv_sem,
            device_id={"frame": lax.rem(frame + 1, 32)},
            device_id_type=MESH,
        )

    row = lax.broadcasted_iota(jnp.int32, (LANES, LANES), 0)
    column = lax.broadcasted_iota(jnp.int32, (LANES, LANES), 1)
    same = lax.rem(row, SLAB) == lax.rem(column, SLAB)
    for i in range(3):
        all_of(
            slab_recv.at[i, pl.ds(1, 31)], slab_send_sem.at[i], slab_recv_sem.at[i]
        ).wait_recv()
        tokens = slab_recv[i].reshape(LANES, 1152)
        for t in range(3):
            projected = jnp.dot(
                tokens, weight[:, 1152 * t : 1152 * t + 1152], preferred_element_type=F32
            ).astype(BF16)
            turned[t] = projected.astype(F32).T
        for n in range(16):
            head = slice(72 * n, 72 * n + 72)
            query = norm_rows(turned[0, head, :], gains[2, :, 0:128]).astype(BF16)
            key = norm_rows(turned[1, head, :], gains[3, :, 0:128]).astype(BF16)
            score = lax.dot_general(
                key, query, (((0,), (0,)), ((), ())), preferred_element_type=F32
            )
            score = jnp.where(same, score * SCORE_SCALE, -1e30)
            expons = jnp.exp2(score - jnp.max(score, axis=0, keepdims=True))
            share = (expons / jnp.sum(expons, axis=0, keepdims=True)).astype(BF16)
            result[head, :] = jnp.dot(
                turned[2, head, :].astype(BF16), share, preferred_element_type=F32
            )
        slab_outgoing[i] = result[...].T.astype(BF16).reshape(32, SLAB, 1152)

        def return_slab(r, carry):
            pltpu.make_async_remote_copy(
                src_ref=slab_outgoing.at[i, r],
                dst_ref=slab_back.at[32 * i + frame],
                send_sem=slab_back_send_sem.at[i],
                recv_sem=slab_back_recv_sem.at[i],
                device_id={"frame": lax.rem(frame + 32 - r, 32)},
                device_id_type=MESH,
            ).start()
            return carry

        lax.fori_loop(1, 32, return_slab, 0)
        slab_back[32 * i + frame] = slab_outgoing[i, 0]

    def store(i):
        return pltpu.make_async_copy(
            staged.at[i], out_ref.at[pl.ds(128 * i, 128)], store_sem.at[i]
        )

    for stage in range(3):
        for r in range(1, 8):
            exchange(stage, lax.rem(me + r, 8), r).wait_send()
    for h in range(2):
        for r in range(1, 8):
            for tile in range(3):
                give_back(h, r, tile).wait_send()
    for i in range(3):
        all_of(
            slab_back.at[pl.ds(32 * i, 31)], slab_back_send_sem.at[i], slab_back_recv_sem.at[i]
        ).wait_recv()
        staged[i] = slab_back[32 * i : 32 * i + 32].reshape(128, 1152)
        store(i).start()
    for i in range(3):
        store(i).wait()
        all_of(
            slab_recv.at[i, pl.ds(1, 31)], slab_send_sem.at[i], slab_recv_sem.at[i]
        ).wait_send()
        all_of(
            slab_back.at[pl.ds(32 * i, 31)], slab_back_send_sem.at[i], slab_back_recv_sem.at[i]
        ).wait_send()


def per_device(
    spatial_qkv,
    residual,
    spatial_gate,
    spatial_proj,
    spatial_qgain,
    spatial_kgain,
    temporal_shift,
    temporal_scale,
    temporal_qkv,
    temporal_qgain,
    temporal_kgain,
):
    vmem = pl.BlockSpec(memory_space=pltpu.VMEM)
    anywhere = pl.BlockSpec(memory_space=pl.ANY)
    dma = pltpu.SemaphoreType.DMA
    split = jnp.transpose(spatial_qkv, (0, 1, 3, 2, 4)).reshape(2, 3, 192, 1152)
    result = pl.pallas_call(
        fused_kernel,
        out_shape=jax.ShapeDtypeStruct((384, 1152), BF16),
        in_specs=[anywhere] * 4 + [vmem] * 7,
        out_specs=anywhere,
        scratch_shapes=[
            pltpu.VMEM((9, 2, 3, 192, LANES), BF16),
            pltpu.VMEM((2, 192, 1152), BF16),
            pltpu.VMEM((1152, 1152), BF16),
            pltpu.VMEM((1152, 3456), BF16),
            pltpu.VMEM((4, 72, 384), F32),
            pltpu.VMEM((3, 1152, 384), F32),
            pltpu.VMEM((16, 3, 72, 384), BF16),
            pltpu.VMEM((2, 8, 3, 72, 384), BF16),
            pltpu.VMEM((2, 72, 1536), BF16),
            pltpu.VMEM((2, 1536, 72), BF16),
            pltpu.VMEM((2, 80, 1536), BF16),
            pltpu.VMEM((2, 1536, 768), F32),
            pltpu.VMEM((2, 8, 72, 384), BF16),
            pltpu.VMEM((16, 72, 384), BF16),
            pltpu.VMEM((96, SLAB, 1152), BF16),
            pltpu.VMEM((3, 32, SLAB, 1152), BF16),
            pltpu.VMEM((3, 1152, LANES), F32),
            pltpu.VMEM((1152, LANES), F32),
            pltpu.VMEM((3, 32, SLAB, 1152), BF16),
            pltpu.VMEM((96, SLAB, 1152), BF16),
            dma((3,)),
            dma((9,)),
            dma((3, 8)),
            dma((3, 8)),
            dma((2, 8, 3)),
            dma((2, 8, 3)),
            dma((3,)),
            dma((3,)),
            dma((3,)),
            dma((3,)),
            pltpu.SemaphoreType.REGULAR((4,)),
            pltpu.VMEM((3, 128, 1152), BF16),
            dma((3,)),
        ],
        compiler_params=pltpu.CompilerParams(
            collective_id=0, has_side_effects=True, vmem_limit_bytes=62 * 1024 * 1024
        ),
        name="fused",
    )(
        split,
        residual.reshape(2, 192, 1152),
        spatial_proj,
        temporal_qkv,
        spatial_gate,
        temporal_shift,
        temporal_scale,
        spatial_qgain.reshape(1, 72),
        spatial_kgain.reshape(1, 72),
        temporal_qgain.reshape(1, 72),
        temporal_kgain.reshape(1, 72),
    )
    return result.reshape(2, 1, 192, 1152)


def solution(mesh):
    return jax.shard_map(
        per_device,
        mesh=mesh,
        in_specs=(
            P(None, "frame", "pos", None, None),
            P(None, "frame", "pos", None),
            P(),
            P(),
            P(),
            P(),
            P(),
            P(),
            P(),
            P(),
            P(),
        ),
        out_specs=P(None, "frame", "pos", None),
        check_vma=False,
    )
```
